32 devices in a mesh: row: 4 (over z), col: 4 (over y, core), rep: 2 (over x).
Axes of the slice: x: 2, y: 2, z: 4, core: 2. Of those that a mesh axis runs over, the one named last changes fastest.
Arguments:
- upstream: float32 [16384, 16384], P('row', ('col', 'rep')), may hold values from -0.046875 to 0.046875
- input_panel: float32 [16384, 1024], P('row', ('col', 'rep')), may hold values from -6 to 6
Outputs:
- panel_grad: float32 [16384, 1024], P('row', ('col', 'rep'))
The draws below stay inside these ranges and needn't reach their ends.
All inputs are finite; a program needn't handle non-finite values.
Results may differ from the reference program's by a relative error of at most 0.000071.
Values sent between devices are 32-bit elements; how exact they have to be, the bound alone decides.
A program may use at most 192 MiB of HBM per device.

```python
import jax
import jax.numpy as jnp
from jax import lax

N = 16384
K = 1024


def block_scale(stream_key, extent, split, least, high):
    def one(dim, parts):
        draws = jax.random.uniform(jax.random.fold_in(jax.random.fold_in(stream_key, 6), dim), (parts,), jnp.float32, least / len(split), high / len(split))
        return jnp.repeat(jnp.exp(draws), extent[dim] // parts).reshape((-1,) + (1,) * (len(extent) - dim - 1))

    level = one(*split[0])
    for cut in split[1:]:
        level = level * one(*cut)
    return level


def scatter_about(key, extent, scale, bound, shards=(), dtype=jnp.bfloat16):
    level = block_scale(key, extent, shards, -0.22, 0.18) if shards else 1.0
    array = jax.random.normal(key, extent, jnp.float32) * scale * level
    return jnp.minimum(jnp.maximum(array, -bound), bound).astype(dtype)


def setup_inputs(seed: int = 0) -> dict:
    streams_of = jax.random.split(jax.random.key(seed), 3)
    upstream = scatter_about(streams_of[0], (N, N), N ** -0.5, 0.046875, ((0, 4), (1, 8)), jnp.float32)
    input_panel = scatter_about(streams_of[1], (N, K), 1.0, 6.0, ((0, 4), (1, 8)), jnp.float32)
    return {"upstream": upstream, "input_panel": input_panel}


def reference(upstream, input_panel):
    precise = lax.Precision.HIGHEST
    lower_tile = jnp.tril(upstream)
    direct = jnp.dot(lower_tile, input_panel, precision=precise, preferred_element_type=jnp.float32)
    mirror = lax.dot_general(lower_tile, input_panel, (((0,), (0,)), ((), ())), precision=precise, preferred_element_type=jnp.float32)
    return direct + mirror
```

```python
import functools

import jax
import jax.numpy as jnp
from jax import lax
from jax.experimental import pallas as pl
from jax.experimental.pallas import tpu as pltpu
from jax.sharding import PartitionSpec as P

GROUP = ("col", "rep")
ALL = ("row", "col", "rep")
MESH = pl.DeviceIdType.MESH
LANES = 128
CHIPS = 4
OFFSETS = (0, 1, 3, 2)
TILE = 512
DEEP = 256

CHUNKS = 4


def product(left, right, contract):
    return lax.dot_general(
        left,
        right,
        (contract, ((), ())),
        precision=lax.Precision.HIGH,
        preferred_element_type=jnp.float32,
    )


def per_device(rows, groups, upstream, input_panel):
    row_count, col_count = upstream.shape
    width = input_panel.shape[1]
    ratio = row_count // col_count
    row_index = lax.axis_index("row")
    col_index = lax.axis_index(GROUP)
    owner = col_index // ratio
    part = (col_index % ratio) * col_count
    rows_global = row_index * row_count + lax.broadcasted_iota(jnp.int32, (row_count, col_count), 0)
    cols_global = col_index * col_count + lax.broadcasted_iota(jnp.int32, (row_count, col_count), 1)
    lower_tile = jnp.where(cols_global <= rows_global, upstream, jnp.float32(0.0))
    panel_t = jnp.transpose(input_panel)
    step = width // CHUNKS

    def hop(value, pairs):
        return lax.ppermute(value, ALL, [(a * groups + g, b * groups + g) for a, b, g in pairs])

    outs = []
    for c in range(CHUNKS):
        band = lax.all_gather(panel_t[c * step : (c + 1) * step], GROUP, axis=0, tiled=True)
        held = lax.dynamic_slice_in_dim(band, part, col_count, 1)
        block = held
        for s in range(rows - 1):
            pairs = [(g // ratio + s, g // ratio + s + 1, g) for g in range(groups) if g // ratio + s + 1 < rows]
            held = hop(held, pairs)
            block = jnp.where(row_index == owner + s + 1, held, block)
        total = product(band, lower_tile, ((1,), (0,)))
        for s in range(rows - 1):
            r = rows - 1 - s
            pairs = [(r, r - 1, g) for g in range(groups) if g // ratio <= r - 1]
            total = total + hop(total, pairs)
        lower = product(block, lower_tile, ((1,), (1,)))
        total = jnp.where(row_index == owner, total, 0.0)
        here = lax.dynamic_slice_in_dim(lower, part, col_count, 1)
        lower = lax.dynamic_update_slice_in_dim(lower, here + total, part, 1)
        outs.append(lax.psum_scatter(lower, GROUP, scatter_dimension=0, tiled=True))
    return jnp.transpose(jnp.concatenate(outs, 0))


def split(value):
    high = value.astype(jnp.bfloat16)
    low = (value - high.astype(jnp.float32)).astype(jnp.bfloat16)
    return high, low


def dot(left, right):
    return jnp.dot(left, right, preferred_element_type=jnp.float32)


def kernel(rows, upstream, panel, out, ag, pg, uin, rs, uf, cx, t0,
           high, low, work, pt, pgb, u,
           ag_send, ag_recv, pg_send, pg_recv, u_send, u_recv, uf_recv,
           cx_send, cx_recv, rs_send, rs_recv, local):
    full, span = upstream.shape
    ratio = full // span
    r = lax.axis_index("row")
    col = lax.axis_index("col")
    x = lax.axis_index("rep")
    y = col // 2
    core = col % 2
    mate = 1 - core
    g = col * 2 + x
    p = 2 * y + (x + y) % 2
    owner = g // ratio
    part = pl.multiple_of((g % ratio) * span, span)
    active = r >= owner
    last = rows - 1

    def place(chip, c):
        return {"col": 2 * (chip // 2) + c, "rep": (chip + chip // 2) % 2}

    def chip_at(d):
        return lax.rem(p + d, CHIPS)

    def remote(src, dst, send, recv, where):
        return pltpu.make_async_remote_copy(
            src_ref=src, dst_ref=dst, send_sem=send, recv_sem=recv, device_id=where, device_id_type=MESH
        )

    mate_at = place(p, mate)
    above = {"row": jnp.minimum(r + 1, last)}
    below = {"row": jnp.maximum(r - 1, 0)}

    slots = 4
    blocks = span // LANES

    def tile_copy(j, slot):
        columns = pl.ds(pl.multiple_of(j * LANES, LANES), LANES)
        return pltpu.make_async_copy(upstream.at[:, columns], work.at[slot], local.at[slot])

    @pl.when(active)
    def _():
        for j in range(slots):
            tile_copy(j, j).start()

    barrier = pltpu.get_barrier_semaphore()
    for d in range(CHIPS):
        for c in (0, 1):
            other = core if c == 0 else mate
            if d == 0 and c == 0:
                continue
            pl.semaphore_signal(barrier, inc=1, device_id=place(chip_at(d), other), device_id_type=MESH)

    @pl.when(r < last)
    def _():
        pl.semaphore_signal(barrier, inc=1, device_id=above, device_id_type=MESH)

    @pl.when(r > 0)
    def _():
        pl.semaphore_signal(barrier, inc=1, device_id=below, device_id_type=MESH)

    pl.semaphore_wait(barrier, 2 * CHIPS - 1 + jnp.minimum(r, 1) + jnp.minimum(last - r, 1))

    def own_send(n, where):
        return remote(panel, ag.at[p, core], ag_send.at[n], ag_recv.at[p, core], where)

    own_sends = [own_send(0, mate_at)]
    own_sends += [own_send(d, place(chip_at(d), core)) for d in (1, 3, 2)]
    for send in own_sends:
        send.start()

    def arrived(d, c):
        q = chip_at(d)
        remote(panel, ag.at[q, c], ag_send.at[0], ag_recv.at[q, c], mate_at).wait_recv()

    def pass_on(d):
        q = chip_at(d)
        return remote(ag.at[q, core], ag.at[q, core], ag_send.at[3 + d], ag_recv.at[q, core], mate_at)

    is_source = jnp.logical_and(r == owner, r < last)
    is_relay = jnp.logical_and(r > owner, r < last)

    def block_send(src, k):
        return remote(src, pg.at[k], pg_send.at[k], pg_recv.at[k], above)

    def source_send(c, own):
        @pl.when(is_source)
        def _():
            q = chip_at(OFFSETS[c])
            if c == 0:
                if own:
                    block_send(panel.at[pl.ds(part, span)], core).start()
                else:
                    block_send(ag.at[q, mate, pl.ds(part, span)], mate).start()
            else:
                for b in (0, 1):
                    block_send(ag.at[q, b, pl.ds(part, span)], 2 * c + b).start()

    def block_wait(k):
        block_send(pg.at[k], k).wait_recv()

    def relay(k):
        @pl.when(is_relay)
        def _():
            block_wait(k)
            block_send(pg.at[k], k).start()

    source_send(0, True)
    arrived(0, mate)
    source_send(0, False)

    @pl.when(active)
    def _():
        @pl.loop(0, blocks)
        def _(j):
            slot = lax.rem(j, slots)
            tile_copy(j, slot).wait()
            columns = pl.ds(pl.multiple_of(j * LANES, LANES), LANES)

            @pl.loop(0, full // TILE)
            def _(i):
                lines = pl.ds(pl.multiple_of(i * TILE, TILE), TILE)
                at = r * full + i * TILE + lax.broadcasted_iota(jnp.int32, (TILE, LANES), 0)
                to = g * span + j * LANES + lax.broadcasted_iota(jnp.int32, (TILE, LANES), 1)
                value = jnp.where(to <= at, work[slot, lines], 0.0)
                big, small = split(value)
                high[lines, columns] = big
                low[lines, columns] = small

            @pl.when(j + slots < blocks)
            def _():
                tile_copy(j + slots, slot).start()

    def mirror(c):
        @pl.when(active)
        def _():
            d = OFFSETS[c]
            q = chip_at(d)
            loads = []
            for b in (0, 1):
                if d == 0:
                    src = panel if b == 0 else ag.at[q, mate]
                    dst = core if b == 0 else mate
                else:
                    src = ag.at[q, b]
                    dst = b
                loads.append(pltpu.make_async_copy(src, work.at[dst], local.at[b]))
            for load in loads:
                load.start()
            for load in loads:
                load.wait()

            @pl.loop(0, full // TILE)
            def _(i):
                lines = pl.ds(pl.multiple_of(i * TILE, TILE), TILE)
                for b in (0, 1):
                    big, small = split(jnp.transpose(work[b, lines]))
                    pt[b * LANES:(b + 1) * LANES, lines] = big
                    pt[(2 + b) * LANES:(3 + b) * LANES, lines] = small

            @pl.loop(0, span // DEEP)
            def _(j):
                columns = pl.ds(pl.multiple_of(j * DEEP, DEEP), DEEP)
                both = dot(pt[...], high[:, columns])
                rest = dot(pt[0:2 * LANES], low[:, columns])
                value = jnp.transpose(both[:2 * LANES] + both[2 * LANES:] + rest)
                u[2 * c, columns] = value[:, :LANES]
                u[2 * c + 1, columns] = value[:, LANES:]

    def down_send(k):
        return remote(u.at[k], uin.at[k], u_send.at[k], u_recv.at[k], below)

    def home_slot():
        return uf.at[pl.ds(part, span)]

    def home_send(k):
        q = chip_at(OFFSETS[k // 2])
        return remote(u.at[k], home_slot(), u_send.at[k], uf_recv.at[g % ratio], place(q, k % 2))

    def home_copy(k):
        return pltpu.make_async_copy(u.at[k], home_slot(), uf_recv.at[g % ratio])

    is_down = r > owner
    is_home = r == owner

    def finish(k):
        @pl.when(is_down)
        def _():
            down_send(k).start()

        if k < 2:
            @pl.when(jnp.logical_and(is_home, core == k))
            def _():
                home_copy(k).start()

            @pl.when(jnp.logical_and(is_home, core != k))
            def _():
                home_send(k).start()
        else:
            @pl.when(is_home)
            def _():
                home_send(k).start()

    def add_arrived(k):
        down_send(k).wait_recv()
        load = pltpu.make_async_copy(uin.at[k], work.at[0, pl.ds(0, span)], local.at[0])
        load.start()
        load.wait()

        @pl.loop(0, span // TILE)
        def _(i):
            lines = pl.ds(pl.multiple_of(i * TILE, TILE), TILE)
            u[k, lines] = u[k, lines] + work[0, lines]

    def duty(step):
        for h in range(rows):
            k = step - h
            if h == 0:
                ks = [k for k in (2 * step, 2 * step + 1) if step < CHIPS]
            else:
                ks = [k] if 0 <= k < 2 * CHIPS else []
            for k in ks:
                @pl.when(jnp.logical_and(r == last - h, active))
                def _(k=k, h=h):
                    if h:
                        add_arrived(k)
                    finish(k)

    def trade(c):
        return remote(work.at[2 + mate], cx.at[c], cx_send.at[c], cx_recv.at[c], mate_at)

    def sum_send(c):
        d = OFFSETS[c]
        return remote(work.at[4 + c % 2], rs.at[d - 1], rs_send.at[d - 1], rs_recv.at[d - 1], place(chip_at(d), core))

    keep = pltpu.make_async_copy(work.at[4], t0, local.at[3])

    def direct(c):
        if c:
            trade(c - 1).wait_send()

        @pl.when(active)
        def _():
            q = chip_at(OFFSETS[c])

            @pl.when(r == last)
            def _():
                @pl.when(is_down)
                def _():
                    for b in (0, 1):
                        block_wait(2 * c + b)

            def load(src, b):
                return pltpu.make_async_copy(src, work.at[0, pl.ds(b * span, span)], local.at[b])

            @pl.when(is_down)
            def _():
                for b in (0, 1):
                    load(pg.at[2 * c + b], b).start()

            @pl.when(is_home)
            def _():
                for b in (0, 1):
                    if c:
                        load(ag.at[q, b, pl.ds(part, span)], b).start()
                    else:
                        @pl.when(core == b)
                        def _(b=b):
                            load(panel.at[pl.ds(part, span)], b).start()

                        @pl.when(core != b)
                        def _(b=b):
                            load(ag.at[q, b, pl.ds(part, span)], b).start()

            for b in (0, 1):
                load(pg.at[0], b).wait()

            @pl.loop(0, span // TILE)
            def _(i):
                lines = pl.ds(pl.multiple_of(i * TILE, TILE), TILE)
                for b in (0, 1):
                    big, small = split(work[0, pl.ds(pl.multiple_of(b * span + i * TILE, TILE), TILE)])
                    pgb[lines, b * LANES:(b + 1) * LANES] = big
                    pgb[lines, (2 + b) * LANES:(3 + b) * LANES] = small

            @pl.loop(0, full // TILE)
            def _(i):
                lines = pl.ds(pl.multiple_of(i * TILE, TILE), TILE)
                both = dot(high[lines], pgb[...])
                rest = dot(low[lines], pgb[:, :2 * LANES])
                value = both[:, :2 * LANES] + both[:, 2 * LANES:] + rest
                work[2, lines] = value[:, :LANES]
                work[3, lines] = value[:, LANES:]

        @pl.when(jnp.logical_not(active))
        def _():
            @pl.loop(0, full // TILE)
            def _(i):
                lines = pl.ds(pl.multiple_of(i * TILE, TILE), TILE)
                work[2, lines] = jnp.zeros((TILE, LANES), jnp.float32)
                work[3, lines] = jnp.zeros((TILE, LANES), jnp.float32)

        trade(c).start()
        trade(c).wait_recv()
        load = pltpu.make_async_copy(cx.at[c], work.at[1], local.at[2])
        load.start()
        load.wait()
        if c == 2:
            keep.wait()
        if c == 3:
            sum_send(1).wait_send()
        slot = 4 + c % 2

        @pl.loop(0, full // TILE)
        def _(i):
            lines = pl.ds(pl.multiple_of(i * TILE, TILE), TILE)
            work[slot, lines] = work[2 + core, lines] + work[1, lines]

        if c == 0:
            keep.start()
        else:
            sum_send(c).start()

    for step in range(2 * CHIPS + rows - 1):
        if step < CHIPS:
            mirror(step)
        elif step < 2 * CHIPS:
            direct(step - CHIPS)
        ready = {0: (1, 2), 2: (3,)}.get(step, ())
        for c in ready:
            arrived(OFFSETS[c], core)
            pass_on(OFFSETS[c]).start()
        for c in ready:
            arrived(OFFSETS[c], mate)
            source_send(c, True)
        if step < 2 * CHIPS - 1:
            relay(step)
        if step == 2 * CHIPS - 2:
            relay(step + 1)
        duty(step)

    trade(CHIPS - 1).wait_send()
    for c in (2, 3):
        sum_send(c).wait_send()
    for d in range(1, CHIPS):
        remote(rs.at[d - 1], rs.at[d - 1], rs_send.at[d - 1], rs_recv.at[d - 1], mate_at).wait_recv()
    for a in range(ratio):
        slot = uf.at[pl.ds(a * span, span)]
        remote(slot, slot, u_send.at[0], uf_recv.at[a], mate_at).wait_recv()
    sources = (t0, rs.at[0], rs.at[1], rs.at[2], uf)
    loads = [pltpu.make_async_copy(src, work.at[n], local.at[n]) for n, src in enumerate(sources)]
    for load in loads:
        load.start()
    for load in loads:
        load.wait()

    @pl.loop(0, full // TILE)
    def _(i):
        lines = pl.ds(pl.multiple_of(i * TILE, TILE), TILE)
        total = work[0, lines] + work[1, lines] + work[2, lines] + work[3, lines] + work[4, lines]
        work[5, lines] = total

    store = pltpu.make_async_copy(work.at[5], out, local.at[5])
    store.start()

    for send in own_sends:
        send.wait_send()
    for d in (1, 3, 2):
        pass_on(d).wait_send()

    @pl.when(jnp.logical_or(is_source, is_relay))
    def _():
        for k in range(2 * CHIPS):
            block_send(pg.at[k], k).wait_send()

    for k in range(2 * CHIPS):
        @pl.when(is_down)
        def _(k=k):
            down_send(k).wait_send()

        sent_home = jnp.logical_and(is_home, core != k) if k < 2 else is_home

        @pl.when(sent_home)
        def _(k=k):
            home_send(k).wait_send()

    store.wait()


def fused(rows, upstream, input_panel):
    full, span = upstream.shape
    width = input_panel.shape[1]
    ratio = full // span
    pieces = 2 * CHIPS
    f32 = jnp.float32
    shapes = [
        (full, width),
        (CHIPS, 2, full, width),
        (pieces, span, width),
        (pieces, span, width),
        (CHIPS - 1, full, width),
        (full, width),
        (CHIPS, full, width),
        (full, width),
    ]
    anywhere = pl.BlockSpec(memory_space=pl.ANY)
    dma = pltpu.SemaphoreType.DMA
    results = pl.pallas_call(
        functools.partial(kernel, rows),
        out_shape=[jax.ShapeDtypeStruct(shape, f32) for shape in shapes],
        in_specs=[anywhere] * 2,
        out_specs=[anywhere] * len(shapes),
        scratch_shapes=[
            pltpu.VMEM((full, span), jnp.bfloat16),
            pltpu.VMEM((full, span), jnp.bfloat16),
            pltpu.VMEM((6, full, width), f32),
            pltpu.VMEM((4 * width, full), jnp.bfloat16),
            pltpu.VMEM((span, 4 * width), jnp.bfloat16),
            pltpu.VMEM((pieces, span, width), f32),
            dma((7,)),
            dma((CHIPS, 2)),
            dma((pieces,)),
            dma((pieces,)),
            dma((pieces,)),
            dma((pieces,)),
            dma((ratio,)),
            dma((CHIPS,)),
            dma((CHIPS,)),
            dma((CHIPS - 1,)),
            dma((CHIPS - 1,)),
            dma((6,)),
        ],
        compiler_params=pltpu.CompilerParams(
            collective_id=0, has_side_effects=True, vmem_limit_bytes=67043328
        ),
    )(upstream, input_panel)
    return results[0]


def solution(mesh):
    rows = mesh.shape["row"]
    cols, reps = mesh.shape["col"], mesh.shape["rep"]
    placed = P("row", GROUP)

    def body(upstream, input_panel):
        full, span = upstream.shape
        whole_tiles = input_panel.shape[1] == LANES and full % TILE == 0 and span % TILE == 0
        if cols == 4 and reps == 2 and full == 2 * span and rows > 1 and whole_tiles:
            return fused(rows, upstream, input_panel)
        return per_device(rows, cols * reps, upstream, input_panel)

    return jax.shard_map(
        body, mesh=mesh, in_specs=(placed, placed), out_specs=placed, check_vma=False
    )
```

```python
import functools

import jax
import jax.numpy as jnp
from jax import lax
from jax.experimental import pallas as pl
from jax.experimental.pallas import tpu as pltpu
from jax.sharding import PartitionSpec as P

GROUP = ("col", "rep")
ALL = ("row", "col", "rep")
MESH = pl.DeviceIdType.MESH
LANES = 128
CHIPS = 4
ORDER = (2, 1, 3, 0)
UPWARD = ((0, 0), (2, 0), (2, 1), (1, 0), (1, 1), (3, 0), (3, 1), (0, 1))
TILE = 512
DEEP = 256

CHUNKS = 4


def product(left, right, contract):
    return lax.dot_general(
        left,
        right,
        (contract, ((), ())),
        precision=lax.Precision.HIGH,
        preferred_element_type=jnp.float32,
    )


def per_device(rows, groups, upstream, input_panel):
    row_count, col_count = upstream.shape
    width = input_panel.shape[1]
    ratio = row_count // col_count
    row_index = lax.axis_index("row")
    col_index = lax.axis_index(GROUP)
    owner = col_index // ratio
    part = (col_index % ratio) * col_count
    rows_global = row_index * row_count + lax.broadcasted_iota(jnp.int32, (row_count, col_count), 0)
    cols_global = col_index * col_count + lax.broadcasted_iota(jnp.int32, (row_count, col_count), 1)
    lower_tile = jnp.where(cols_global <= rows_global, upstream, jnp.float32(0.0))
    panel_t = jnp.transpose(input_panel)
    step = width // CHUNKS

    def hop(value, pairs):
        return lax.ppermute(value, ALL, [(a * groups + g, b * groups + g) for a, b, g in pairs])

    outs = []
    for c in range(CHUNKS):
        band = lax.all_gather(panel_t[c * step : (c + 1) * step], GROUP, axis=0, tiled=True)
        held = lax.dynamic_slice_in_dim(band, part, col_count, 1)
        block = held
        for s in range(rows - 1):
            pairs = [(g // ratio + s, g // ratio + s + 1, g) for g in range(groups) if g // ratio + s + 1 < rows]
            held = hop(held, pairs)
            block = jnp.where(row_index == owner + s + 1, held, block)
        total = product(band, lower_tile, ((1,), (0,)))
        for s in range(rows - 1):
            r = rows - 1 - s
            pairs = [(r, r - 1, g) for g in range(groups) if g // ratio <= r - 1]
            total = total + hop(total, pairs)
        lower = product(block, lower_tile, ((1,), (1,)))
        total = jnp.where(row_index == owner, total, 0.0)
        here = lax.dynamic_slice_in_dim(lower, part, col_count, 1)
        lower = lax.dynamic_update_slice_in_dim(lower, here + total, part, 1)
        outs.append(lax.psum_scatter(lower, GROUP, scatter_dimension=0, tiled=True))
    return jnp.transpose(jnp.concatenate(outs, 0))


def split(value):
    high = value.astype(jnp.bfloat16)
    low = (value - high.astype(jnp.float32)).astype(jnp.bfloat16)
    return high, low


def dot(left, right):
    return jnp.dot(left, right, preferred_element_type=jnp.float32)


def kernel(rows, upstream, panel, out, ag, pg, uin, rs, uf, cx,
           high, low, work, pt, pgb, u,
           ag_send, ag_recv, pg_send, pg_recv, u_send, u_recv, home_sem, uf_recv,
           cx_send, cx_recv, rs_send, rs_recv, local):
    full, span = upstream.shape
    ratio = full // span
    r = lax.axis_index("row")
    col = lax.axis_index("col")
    x = lax.axis_index("rep")
    y = col // 2
    core = col % 2
    mate = 1 - core
    g = col * 2 + x
    p = 2 * y + x
    owner = g // ratio
    part = pl.multiple_of((g % ratio) * span, span)
    active = r >= owner
    last = rows - 1

    def place(chip, c):
        return {"col": 2 * (chip // 2) + c, "rep": chip % 2}

    def chip_at(d):
        across = 1 - x if d % 2 else x
        along = 1 - y if d // 2 else y
        return 2 * along + across

    def remote(src, dst, send, recv, where):
        return pltpu.make_async_remote_copy(
            src_ref=src, dst_ref=dst, send_sem=send, recv_sem=recv, device_id=where, device_id_type=MESH
        )

    mate_at = place(p, mate)
    above = {"row": jnp.minimum(r + 1, last)}
    below = {"row": jnp.maximum(r - 1, 0)}

    slots = 4
    blocks = span // LANES

    def tile_copy(j, slot):
        columns = pl.ds(pl.multiple_of(j * LANES, LANES), LANES)
        return pltpu.make_async_copy(upstream.at[:, columns], work.at[slot], local.at[slot])

    @pl.when(active)
    def _():
        for j in range(slots):
            tile_copy(j, j).start()

    barrier = pltpu.get_barrier_semaphore()
    for d in range(CHIPS):
        for c in (0, 1):
            other = core if c == 0 else mate
            if d == 0 and c == 0:
                continue
            pl.semaphore_signal(barrier, inc=1, device_id=place(chip_at(d), other), device_id_type=MESH)

    @pl.when(r < last)
    def _():
        pl.semaphore_signal(barrier, inc=1, device_id=above, device_id_type=MESH)

    @pl.when(r > 0)
    def _():
        pl.semaphore_signal(barrier, inc=1, device_id=below, device_id_type=MESH)

    pl.semaphore_wait(barrier, 2 * CHIPS - 1 + jnp.minimum(r, 1) + jnp.minimum(last - r, 1))

    def half(x_to, h):
        at = x_to if h == 0 else 1 - x_to
        return pl.ds(pl.multiple_of(at * span, span), span)

    def own_send(d, h):
        to = mate_at if d == 0 else place(chip_at(d), core)
        lines = half(to["rep"], h)
        return remote(panel.at[lines], ag.at[p, core, lines], ag_send.at[d, h], ag_recv.at[p, core, h], to)

    own_order = ((0, 0), (0, 1), (2, 0), (1, 0), (2, 1), (1, 1), (3, 0), (3, 1))
    for d, h in own_order:
        own_send(d, h).start()

    def arrived(d, c, h):
        q = chip_at(d)
        view = ag.at[q, c, half(x, h)]
        remote(view, view, ag_send.at[0, 0], ag_recv.at[q, c, h], mate_at).wait_recv()

    def pass_on(d, h):
        q = chip_at(d)
        view = ag.at[q, core, half(x, h)]
        return remote(view, view, ag_send.at[3 + d, h], ag_recv.at[q, core, h], mate_at)

    def gather(offsets, h):
        for d in offsets:
            arrived(d, core, h)
            pass_on(d, h).start()
        for d in offsets:
            arrived(d, mate, h)

    is_source = jnp.logical_and(r == owner, r < last)
    is_relay = jnp.logical_and(r > owner, r < last)

    def block_send(src, k):
        return remote(src, pg.at[k], pg_send.at[k], pg_recv.at[k], above)

    def source_send(k):
        c, b = UPWARD[k]
        q = chip_at(c)
        lines = pl.ds(part, span)

        if c:
            @pl.when(is_source)
            def _():
                block_send(ag.at[q, b, lines], k).start()
        else:
            @pl.when(jnp.logical_and(is_source, core == b))
            def _():
                block_send(panel.at[lines], k).start()

            @pl.when(jnp.logical_and(is_source, core != b))
            def _():
                block_send(ag.at[q, b, lines], k).start()

    def block_wait(k):
        block_send(pg.at[k], k).wait_recv()

    def relay(k):
        @pl.when(is_relay)
        def _():
            block_wait(k)
            block_send(pg.at[k], k).start()

    arrived(0, mate, 0)
    source_send(0)
    arrived(0, mate, 1)

    @pl.when(active)
    def _():
        @pl.loop(0, blocks)
        def _(j):
            slot = lax.rem(j, slots)
            tile_copy(j, slot).wait()
            columns = pl.ds(pl.multiple_of(j * LANES, LANES), LANES)

            @pl.loop(0, full // TILE)
            def _(i):
                lines = pl.ds(pl.multiple_of(i * TILE, TILE), TILE)
                at = r * full + i * TILE + lax.broadcasted_iota(jnp.int32, (TILE, LANES), 0)
                to = g * span + j * LANES + lax.broadcasted_iota(jnp.int32, (TILE, LANES), 1)
                value = jnp.where(to <= at, work[slot, lines], 0.0)
                big, small = split(value)
                high[lines, columns] = big
                low[lines, columns] = small

            @pl.when(j + slots < blocks)
            def _():
                tile_copy(j + slots, slot).start()

    @pl.when(jnp.logical_not(active))
    def _():
        @pl.loop(0, full // TILE)
        def _(i):
            lines = pl.ds(pl.multiple_of(i * TILE, TILE), TILE)
            work[2, lines] = jnp.zeros((TILE, LANES), jnp.float32)
            work[3, lines] = jnp.zeros((TILE, LANES), jnp.float32)

    def mirror_load(c):
        @pl.when(active)
        def _():
            d = c
            q = chip_at(d)
            loads = []
            for b in (0, 1):
                if d == 0:
                    src = panel if b == 0 else ag.at[q, mate]
                    dst = core if b == 0 else mate
                else:
                    src = ag.at[q, b]
                    dst = b
                loads.append(pltpu.make_async_copy(src, work.at[dst], local.at[b]))
            for load in loads:
                load.start()
            for load in loads:
                load.wait()

            @pl.loop(0, full // TILE)
            def _(i):
                lines = pl.ds(pl.multiple_of(i * TILE, TILE), TILE)
                for b in (0, 1):
                    big, small = split(jnp.transpose(work[b, lines]))
                    pt[b * LANES:(b + 1) * LANES, lines] = big
                    pt[(2 + b) * LANES:(3 + b) * LANES, lines] = small

    def mirror(c, h):
        @pl.when(active)
        def _():
            steps = span // DEEP // 2

            @pl.loop(h * steps, (h + 1) * steps)
            def _(j):
                columns = pl.ds(pl.multiple_of(j * DEEP, DEEP), DEEP)
                both = dot(pt[...], high[:, columns])
                rest = dot(pt[0:2 * LANES], low[:, columns])
                value = jnp.transpose(both[:2 * LANES] + both[2 * LANES:] + rest)
                lines = pl.ds(pl.multiple_of((j - h * steps) * DEEP, DEEP), DEEP)
                for b in (0, 1):
                    u[2 * c + h, b, lines] = value[:, b * LANES:(b + 1) * LANES]

    def down_send(k):
        return remote(u.at[k], uin.at[k], u_send.at[k], u_recv.at[k], below)

    def home_slot(k):
        return uf.at[pl.ds(pl.multiple_of(part + (k % 2) * (span // 2), span // 2), span // 2)]

    def home_recv(k):
        return uf_recv.at[g % ratio, k % 2]

    def home_send(k, b):
        to = place(chip_at(k // 2), b)
        return remote(u.at[k, b], home_slot(k), home_sem.at[k, b], home_recv(k), to)

    def home_copy(k, b):
        return pltpu.make_async_copy(u.at[k, b], home_slot(k), home_recv(k))

    is_down = r > owner
    is_home = r == owner

    def finish(k):
        @pl.when(is_down)
        def _():
            down_send(k).start()

        for b in (0, 1):
            if k // 2:
                @pl.when(is_home)
                def _(b=b):
                    home_send(k, b).start()
            else:
                @pl.when(jnp.logical_and(is_home, core == b))
                def _(b=b):
                    home_copy(k, b).start()

                @pl.when(jnp.logical_and(is_home, core != b))
                def _(b=b):
                    home_send(k, b).start()

    def add_arrived(k):
        down_send(k).wait_recv()
        loads = [
            pltpu.make_async_copy(uin.at[k, b], work.at[0, pl.ds(b * (span // 2), span // 2)], local.at[b])
            for b in (0, 1)
        ]
        for load in loads:
            load.start()
        for load in loads:
            load.wait()

        @pl.loop(0, span // 2 // TILE)
        def _(i):
            for b in (0, 1):
                lines = pl.ds(pl.multiple_of(i * TILE, TILE), TILE)
                other = pl.ds(pl.multiple_of(b * (span // 2) + i * TILE, TILE), TILE)
                u[k, b, lines] = u[k, b, lines] + work[0, other]

    def relay_slot(row, k):
        if row == 1:
            return (0, 2, 3, 5, 6, 7, 8, 9)[k]
        return min((2, 4, 6, 8, 10, 12, 13, 14)[k] + 2 * (row - 2), (7, 7, 7, 11, 11, 13, 13, 15)[k])

    def duty_slot(h, k):
        if h == 0:
            return (1, 2, 4, 5, 6, 7, 10, 11)[k]
        if h == 1:
            return (3, 5, 7, 9, 11, 13, 14, 16)[k]
        return (5, 7, 9, 11, 14, 15, 17, 18)[k] if h == 2 else (7, 9, 11, 12, 15, 16, 18, 19)[k] + h - 3

    def service(slot):
        for k in range(2 * CHIPS):
            if duty_slot(0, k) == slot:
                @pl.when(r == last)
                def _(k=k):
                    finish(k)
        if slot == 1:
            gather((1, 2), 0)
            for k in (1, 2, 3, 4):
                source_send(k)
        if slot == 5:
            gather((3,), 0)
            for k in (5, 6, 7):
                source_send(k)
        for h in range(1, rows):
            for k in range(2 * CHIPS):
                if duty_slot(h, k) == slot:
                    @pl.when(jnp.logical_and(r == last - h, active))
                    def _(k=k):
                        add_arrived(k)
                        finish(k)
        for row in range(1, last):
            for k in range(2 * CHIPS):
                if relay_slot(row, k) == slot:
                    @pl.when(r == row)
                    def _(k=k):
                        relay(k)
        if slot == 2:
            gather((1, 2), 1)
        if slot == 7:
            gather((3,), 1)

    def rows_half(h):
        return pl.ds(h * (full // 2), full // 2)

    def trade(c, h):
        lines = rows_half(h)
        return remote(work.at[2 + mate, lines], cx.at[c, lines], cx_send.at[c, h], cx_recv.at[c, h], mate_at)

    def sum_send(c, h):
        d = c
        lines = rows_half(h)
        return remote(
            work.at[4 + ORDER.index(c) % 2, lines], rs.at[d - 1, lines],
            rs_send.at[d - 1, h], rs_recv.at[d - 1, h], place(chip_at(d), core),
        )

    def direct_load(t):
        c = ORDER[t]

        @pl.when(active)
        def _():
            q = chip_at(c)

            @pl.when(jnp.logical_and(r == last, is_down))
            def _():
                for k in range(2 * CHIPS):
                    if UPWARD[k][0] == c:
                        block_wait(k)

            def load(src, b):
                return pltpu.make_async_copy(src, work.at[0, pl.ds(b * span, span)], local.at[b])

            @pl.when(is_down)
            def _():
                for b in (0, 1):
                    load(pg.at[UPWARD.index((c, b))], b).start()

            @pl.when(is_home)
            def _():
                for b in (0, 1):
                    if c:
                        load(ag.at[q, b, pl.ds(part, span)], b).start()
                    else:
                        @pl.when(core == b)
                        def _(b=b):
                            load(panel.at[pl.ds(part, span)], b).start()

                        @pl.when(core != b)
                        def _(b=b):
                            load(ag.at[q, b, pl.ds(part, span)], b).start()

            for b in (0, 1):
                load(pg.at[0], b).wait()

            @pl.loop(0, span // TILE)
            def _(i):
                lines = pl.ds(pl.multiple_of(i * TILE, TILE), TILE)
                for b in (0, 1):
                    big, small = split(work[0, pl.ds(pl.multiple_of(b * span + i * TILE, TILE), TILE)])
                    pgb[lines, b * LANES:(b + 1) * LANES] = big
                    pgb[lines, (2 + b) * LANES:(3 + b) * LANES] = small

        if t:
            for h in (0, 1):
                trade(ORDER[t - 1], h).wait_send()

    def direct(c, h):
        @pl.when(active)
        def _():
            steps = full // TILE // 2

            @pl.loop(h * steps, (h + 1) * steps)
            def _(i):
                lines = pl.ds(pl.multiple_of(i * TILE, TILE), TILE)
                both = dot(high[lines], pgb[...])
                rest = dot(low[lines], pgb[:, :2 * LANES])
                value = both[:, :2 * LANES] + both[:, 2 * LANES:] + rest
                work[2, lines] = value[:, :LANES]
                work[3, lines] = value[:, LANES:]

        trade(c, h).start()

    def direct_sum(t):
        c = ORDER[t]
        slot = 4 + t % 2 if c else 2 + core
        for h in (0, 1):
            if t == 2:
                sum_send(ORDER[0], h).wait_send()
            trade(c, h).wait_recv()
            load = pltpu.make_async_copy(cx.at[c, rows_half(h)], work.at[1, rows_half(h)], local.at[2])
            load.start()
            load.wait()
            steps = full // TILE // 2

            @pl.loop(h * steps, (h + 1) * steps)
            def _(i):
                lines = pl.ds(pl.multiple_of(i * TILE, TILE), TILE)
                work[slot, lines] = work[2 + core, lines] + work[1, lines]

            if c:
                sum_send(c, h).start()

    service(0)
    tasks = (("m", 0), ("m", 1), ("m", 2), ("d", 0), ("m", 3), ("d", 1), ("d", 2), ("d", 3))
    for i, (kind, n) in enumerate(tasks):
        if kind == "m":
            mirror_load(n)
        else:
            direct_load(n)
        for h in (0, 1):
            if kind == "m":
                mirror(n, h)
            else:
                c = ORDER[n]
                direct(c, h)
                if h:
                    direct_sum(n)
            service(2 * i + h + (2 if i else 1))
        if i == 0:
            service(3)
    for slot in range(4 * CHIPS + 2, 4 * CHIPS + 2 + rows):
        service(slot)

    def add_up(sources):
        loads = [pltpu.make_async_copy(src, work.at[n], local.at[n]) for n, src in enumerate(sources)]
        for load in loads:
            load.start()
        for load in loads:
            load.wait()

        @pl.loop(0, full // TILE)
        def _(i):
            lines = pl.ds(pl.multiple_of(i * TILE, TILE), TILE)
            total = work[2 + core, lines]
            for n in range(len(sources)):
                total = total + work[n, lines]
            work[2 + core, lines] = total

    def sum_wait(d):
        for h in (0, 1):
            view = rs.at[d - 1, rows_half(h)]
            remote(view, view, rs_send.at[d - 1, h], rs_recv.at[d - 1, h], mate_at).wait_recv()

    for h in (0, 1):
        trade(ORDER[-1], h).wait_send()
    sum_wait(1)
    sum_wait(2)
    add_up((rs.at[0], rs.at[1]))
    sum_wait(3)
    add_up((rs.at[2],))
    for a in range(ratio):
        for h in (0, 1):
            view = uf.at[pl.ds(a * span + h * (span // 2), span // 2)]
            remote(view, view, home_sem.at[0, 0], uf_recv.at[a, h], mate_at).wait_recv()
    add_up((uf,))
    store = pltpu.make_async_copy(work.at[2 + core], out, local.at[5])
    store.start()

    for d, h in own_order:
        own_send(d, h).wait_send()
    for d in (1, 2, 3):
        for h in (0, 1):
            pass_on(d, h).wait_send()
    for h in (0, 1):
        sum_send(ORDER[1], h).wait_send()
        sum_send(ORDER[2], h).wait_send()

    @pl.when(jnp.logical_or(is_source, is_relay))
    def _():
        for k in range(2 * CHIPS):
            block_send(pg.at[k], k).wait_send()

    for k in range(2 * CHIPS):
        @pl.when(is_down)
        def _(k=k):
            down_send(k).wait_send()

        for b in (0, 1):
            sent_home = is_home if k // 2 else jnp.logical_and(is_home, core != b)

            @pl.when(sent_home)
            def _(k=k, b=b):
                home_send(k, b).wait_send()

    store.wait()


def fused(rows, upstream, input_panel):
    full, span = upstream.shape
    width = input_panel.shape[1]
    ratio = full // span
    pieces = 2 * CHIPS
    f32 = jnp.float32
    shapes = [
        (full, width),
        (CHIPS, 2, full, width),
        (pieces, span, width),
        (pieces, 2, span // 2, width),
        (CHIPS - 1, full, width),
        (full, width),
        (CHIPS, full, width),
    ]
    anywhere = pl.BlockSpec(memory_space=pl.ANY)
    dma = pltpu.SemaphoreType.DMA
    results = pl.pallas_call(
        functools.partial(kernel, rows),
        out_shape=[jax.ShapeDtypeStruct(shape, f32) for shape in shapes],
        in_specs=[anywhere] * 2,
        out_specs=[anywhere] * len(shapes),
        scratch_shapes=[
            pltpu.VMEM((full, span), jnp.bfloat16),
            pltpu.VMEM((full, span), jnp.bfloat16),
            pltpu.VMEM((6, full, width), f32),
            pltpu.VMEM((4 * width, full), jnp.bfloat16),
            pltpu.VMEM((span, 4 * width), jnp.bfloat16),
            pltpu.VMEM((pieces, 2, span // 2, width), f32),
            dma((7, 2)),
            dma((CHIPS, 2, 2)),
            dma((pieces,)),
            dma((pieces,)),
            dma((pieces,)),
            dma((pieces,)),
            dma((pieces, 2)),
            dma((ratio, 2)),
            dma((CHIPS, 2)),
            dma((CHIPS, 2)),
            dma((CHIPS - 1, 2)),
            dma((CHIPS - 1, 2)),
            dma((6,)),
        ],
        compiler_params=pltpu.CompilerParams(
            collective_id=0, has_side_effects=True, vmem_limit_bytes=67043328
        ),
    )(upstream, input_panel)
    return results[0]


def solution(mesh):
    rows = mesh.shape["row"]
    cols, reps = mesh.shape["col"], mesh.shape["rep"]
    placed = P("row", GROUP)

    def body(upstream, input_panel):
        full, span = upstream.shape
        whole_tiles = input_panel.shape[1] == LANES and full % TILE == 0 and span % (2 * TILE) == 0
        if cols == 4 and reps == 2 and full == 2 * span and rows > 1 and whole_tiles:
            return fused(rows, upstream, input_panel)
        return per_device(rows, cols * reps, upstream, input_panel)

    return jax.shard_map(
        body, mesh=mesh, in_specs=(placed, placed), out_specs=placed, check_vma=False
    )
```

```python
import functools

import jax
import jax.numpy as jnp
from jax import lax
from jax.experimental import pallas as pl
from jax.experimental.pallas import tpu as pltpu
from jax.sharding import PartitionSpec as P

GROUP = ("col", "rep")
ALL = ("row", "col", "rep")
MESH = pl.DeviceIdType.MESH
LANES = 128
CHIPS = 4
ORDER = (2, 1, 3, 0)
UPWARD = ((0, 0), (2, 0), (2, 1), (1, 0), (1, 1), (3, 0), (3, 1), (0, 1))
TILE = 512
DEEP = 256

CHUNKS = 4


def product(left, right, contract):
    return lax.dot_general(
        left,
        right,
        (contract, ((), ())),
        precision=lax.Precision.HIGH,
        preferred_element_type=jnp.float32,
    )


def per_device(rows, groups, upstream, input_panel):
    row_count, col_count = upstream.shape
    width = input_panel.shape[1]
    ratio = row_count // col_count
    row_index = lax.axis_index("row")
    col_index = lax.axis_index(GROUP)
    owner = col_index // ratio
    part = (col_index % ratio) * col_count
    rows_global = row_index * row_count + lax.broadcasted_iota(jnp.int32, (row_count, col_count), 0)
    cols_global = col_index * col_count + lax.broadcasted_iota(jnp.int32, (row_count, col_count), 1)
    lower_tile = jnp.where(cols_global <= rows_global, upstream, jnp.float32(0.0))
    panel_t = jnp.transpose(input_panel)
    step = width // CHUNKS

    def hop(value, pairs):
        return lax.ppermute(value, ALL, [(a * groups + g, b * groups + g) for a, b, g in pairs])

    outs = []
    for c in range(CHUNKS):
        band = lax.all_gather(panel_t[c * step : (c + 1) * step], GROUP, axis=0, tiled=True)
        held = lax.dynamic_slice_in_dim(band, part, col_count, 1)
        block = held
        for s in range(rows - 1):
            pairs = [(g // ratio + s, g // ratio + s + 1, g) for g in range(groups) if g // ratio + s + 1 < rows]
            held = hop(held, pairs)
            block = jnp.where(row_index == owner + s + 1, held, block)
        total = product(band, lower_tile, ((1,), (0,)))
        for s in range(rows - 1):
            r = rows - 1 - s
            pairs = [(r, r - 1, g) for g in range(groups) if g // ratio <= r - 1]
            total = total + hop(total, pairs)
        lower = product(block, lower_tile, ((1,), (1,)))
        total = jnp.where(row_index == owner, total, 0.0)
        here = lax.dynamic_slice_in_dim(lower, part, col_count, 1)
        lower = lax.dynamic_update_slice_in_dim(lower, here + total, part, 1)
        outs.append(lax.psum_scatter(lower, GROUP, scatter_dimension=0, tiled=True))
    return jnp.transpose(jnp.concatenate(outs, 0))


def split(value):
    high = value.astype(jnp.bfloat16)
    low = (value - high.astype(jnp.float32)).astype(jnp.bfloat16)
    return high, low


def dot(left, right):
    return jnp.dot(left, right, preferred_element_type=jnp.float32)


def kernel(rows, upstream, panel, out, ag, pg, uin, rs, uf, cx,
           high, low, work, pt, pgb, u,
           ag_send, ag_recv, pg_send, pg_recv, u_send, u_recv, home_sem, uf_recv,
           cx_send, cx_recv, rs_send, rs_recv, local):
    full, span = upstream.shape
    ratio = full // span
    r = lax.axis_index("row")
    col = lax.axis_index("col")
    x = lax.axis_index("rep")
    y = col // 2
    core = col % 2
    mate = 1 - core
    g = col * 2 + x
    p = 2 * y + x
    owner = g // ratio
    part = pl.multiple_of((g % ratio) * span, span)
    active = r >= owner
    last = rows - 1

    def place(chip, c):
        return {"col": 2 * (chip // 2) + c, "rep": chip % 2}

    def chip_at(d):
        across = x + (d % 2) * (1 - 2 * x)
        along = y + (d // 2) * (1 - 2 * y)
        return 2 * along + across

    def remote(src, dst, send, recv, where):
        return pltpu.make_async_remote_copy(
            src_ref=src, dst_ref=dst, send_sem=send, recv_sem=recv, device_id=where, device_id_type=MESH
        )

    mate_at = place(p, mate)
    above = {"row": jnp.minimum(r + 1, last)}
    below = {"row": jnp.maximum(r - 1, 0)}

    slots = 4
    blocks = span // LANES

    def tile_copy(j, slot):
        columns = pl.ds(pl.multiple_of(j * LANES, LANES), LANES)
        return pltpu.make_async_copy(upstream.at[:, columns], work.at[slot], local.at[slot])

    @pl.when(active)
    def _():
        for j in range(slots):
            tile_copy(j, j).start()

    barrier = pltpu.get_barrier_semaphore()
    for d in range(CHIPS):
        for c in (0, 1):
            other = core if c == 0 else mate
            if d == 0 and c == 0:
                continue
            pl.semaphore_signal(barrier, inc=1, device_id=place(chip_at(d), other), device_id_type=MESH)

    @pl.when(r < last)
    def _():
        pl.semaphore_signal(barrier, inc=1, device_id=above, device_id_type=MESH)

    @pl.when(r > 0)
    def _():
        pl.semaphore_signal(barrier, inc=1, device_id=below, device_id_type=MESH)

    pl.semaphore_wait(barrier, 2 * CHIPS - 1 + jnp.minimum(r, 1) + jnp.minimum(last - r, 1))

    def half(x_to, h):
        at = x_to if h == 0 else 1 - x_to
        return pl.ds(pl.multiple_of(at * span, span), span)

    def own_send(d, h):
        to = mate_at if d == 0 else place(chip_at(d), core)
        lines = half(to["rep"], h)
        return remote(panel.at[lines], ag.at[p, core, lines], ag_send.at[d, h], ag_recv.at[p, core, h], to)

    own_order = ((0, 0), (0, 1), (2, 0), (1, 0), (2, 1), (1, 1), (3, 0), (3, 1))
    for d, h in own_order:
        own_send(d, h).start()

    def arrived(d, c, h):
        q = chip_at(d)
        view = ag.at[q, c, half(x, h)]
        remote(view, view, ag_send.at[0, 0], ag_recv.at[q, c, h], mate_at).wait_recv()

    def pass_on(d, h):
        q = chip_at(d)
        view = ag.at[q, core, half(x, h)]
        return remote(view, view, ag_send.at[3 + d, h], ag_recv.at[q, core, h], mate_at)

    def gather(offsets, h):
        for d in offsets:
            arrived(d, core, h)
            pass_on(d, h).start()
        for d in offsets:
            arrived(d, mate, h)

    is_source = jnp.logical_and(r == owner, r < last)
    is_relay = jnp.logical_and(r > owner, r < last)

    def block_send(src, k):
        return remote(src, pg.at[k], pg_send.at[k], pg_recv.at[k], above)

    def source_send(k):
        c, b = UPWARD[k]
        q = chip_at(c)
        lines = pl.ds(part, span)

        if c:
            @pl.when(is_source)
            def _():
                block_send(ag.at[q, b, lines], k).start()
        else:
            @pl.when(jnp.logical_and(is_source, core == b))
            def _():
                block_send(panel.at[lines], k).start()

            @pl.when(jnp.logical_and(is_source, core != b))
            def _():
                block_send(ag.at[q, b, lines], k).start()

    def block_wait(k):
        block_send(pg.at[k], k).wait_recv()

    def relay(k):
        @pl.when(is_relay)
        def _():
            block_wait(k)
            block_send(pg.at[k], k).start()

    arrived(0, mate, 0)
    source_send(0)
    arrived(0, mate, 1)

    @pl.when(active)
    def _():
        @pl.loop(0, blocks)
        def _(j):
            slot = lax.rem(j, slots)
            tile_copy(j, slot).wait()
            columns = pl.ds(pl.multiple_of(j * LANES, LANES), LANES)

            @pl.loop(0, full // TILE)
            def _(i):
                lines = pl.ds(pl.multiple_of(i * TILE, TILE), TILE)
                at = r * full + i * TILE + lax.broadcasted_iota(jnp.int32, (TILE, LANES), 0)
                to = g * span + j * LANES + lax.broadcasted_iota(jnp.int32, (TILE, LANES), 1)
                value = jnp.where(to <= at, work[slot, lines], 0.0)
                big, small = split(value)
                high[lines, columns] = big
                low[lines, columns] = small

            @pl.when(j + slots < blocks)
            def _():
                tile_copy(j + slots, slot).start()

    @pl.when(jnp.logical_not(active))
    def _():
        @pl.loop(0, full // TILE)
        def _(i):
            lines = pl.ds(pl.multiple_of(i * TILE, TILE), TILE)
            work[2, lines] = jnp.zeros((TILE, LANES), jnp.float32)
            work[3, lines] = jnp.zeros((TILE, LANES), jnp.float32)

    def mirror_load(c):
        @pl.when(active)
        def _():
            d = c
            q = chip_at(d)
            loads = []
            for b in (0, 1):
                if isinstance(d, int) and d == 0:
                    src = panel if b == 0 else ag.at[q, mate]
                    dst = core if b == 0 else mate
                else:
                    src = ag.at[q, b]
                    dst = b
                loads.append(pltpu.make_async_copy(src, work.at[dst], local.at[b]))
            for load in loads:
                load.start()
            for load in loads:
                load.wait()

            @pl.loop(0, full // TILE)
            def _(i):
                lines = pl.ds(pl.multiple_of(i * TILE, TILE), TILE)
                for b in (0, 1):
                    big, small = split(jnp.transpose(work[b, lines]))
                    pt[b * LANES:(b + 1) * LANES, lines] = big
                    pt[(2 + b) * LANES:(3 + b) * LANES, lines] = small

    def mirror(c, h):
        @pl.when(active)
        def _():
            steps = span // DEEP // 2

            @pl.loop(h * steps, (h + 1) * steps)
            def _(j):
                columns = pl.ds(pl.multiple_of(j * DEEP, DEEP), DEEP)
                both = dot(pt[...], high[:, columns])
                rest = dot(pt[0:2 * LANES], low[:, columns])
                value = jnp.transpose(both[:2 * LANES] + both[2 * LANES:] + rest)
                lines = pl.ds(pl.multiple_of((j - h * steps) * DEEP, DEEP), DEEP)
                for b in (0, 1):
                    u[2 * c + h, b, lines] = value[:, b * LANES:(b + 1) * LANES]

    def down_send(k, b):
        return remote(u.at[k, b], uin.at[k, b], u_send.at[k, b], u_recv.at[k, b], below)

    def home_slot(k):
        return uf.at[pl.ds(pl.multiple_of(part + (k % 2) * (span // 2), span // 2), span // 2)]

    def home_recv(k):
        return uf_recv.at[g % ratio, k % 2]

    def home_send(k, b):
        to = place(chip_at(k // 2), b)
        return remote(u.at[k, b], home_slot(k), home_sem.at[k, b], home_recv(k), to)

    def home_copy(k, b):
        return pltpu.make_async_copy(u.at[k, b], home_slot(k), home_recv(k))

    is_down = r > owner
    is_home = r == owner

    def finish(k, b):
        @pl.when(is_down)
        def _():
            down_send(k, b).start()

        if k // 2:
            @pl.when(is_home)
            def _():
                home_send(k, b).start()
        else:
            @pl.when(jnp.logical_and(is_home, core == b))
            def _():
                home_copy(k, b).start()

            @pl.when(jnp.logical_and(is_home, core != b))
            def _():
                home_send(k, b).start()

    def add_arrived(k, b):
        down_send(k, b).wait_recv()
        lines = pl.ds(b * (span // 2), span // 2)
        load = pltpu.make_async_copy(uin.at[k, b], work.at[0, lines], local.at[b])
        load.start()
        load.wait()

        @pl.loop(0, span // 2 // TILE)
        def _(i):
            lines = pl.ds(pl.multiple_of(i * TILE, TILE), TILE)
            other = pl.ds(pl.multiple_of(b * (span // 2) + i * TILE, TILE), TILE)
            u[k, b, lines] = u[k, b, lines] + work[0, other]

    def relay_slot(row, k):
        if row == 1:
            return (0, 2, 3, 5, 6, 7, 8, 9)[k]
        return min((2, 4, 6, 8, 10, 12, 13, 14)[k] + 2 * (row - 2), (7, 7, 7, 11, 11, 13, 13, 15)[k])

    def duty_slot(h, k):
        if h == 0:
            return (1, 2, 4, 5, 6, 7, 10, 11)[k]
        if h == 1:
            return (3, 5, 7, 9, 11, 13, 14, 16)[k]
        return (5, 7, 9, 11, 14, 15, 17, 18)[k] if h == 2 else (7, 9, 11, 12, 15, 16, 18, 19)[k] + h - 3

    def service(slot):
        for k in range(2 * CHIPS):
            if duty_slot(0, k) == slot:
                @pl.when(r == last)
                def _(k=k):
                    for b in (0, 1):
                        finish(k, b)
        if slot == 1:
            gather((1, 2), 0)
            for k in (1, 2, 3, 4):
                source_send(k)
        if slot == 5:
            gather((3,), 0)
            for k in (5, 6, 7):
                source_send(k)
        for h in range(1, rows):
            for k in range(2 * CHIPS):
                if duty_slot(h, k) == slot:
                    @pl.when(jnp.logical_and(r == last - h, active))
                    def _(k=k):
                        for b in (0, 1):
                            add_arrived(k, b)
                            finish(k, b)
        for row in range(1, last):
            for k in range(2 * CHIPS):
                if relay_slot(row, k) == slot:
                    @pl.when(r == row)
                    def _(k=k):
                        relay(k)
        if slot == 2:
            gather((1, 2), 1)
        if slot == 7:
            gather((3,), 1)

    def rows_half(h):
        return pl.ds(h * (full // 2), full // 2)

    def trade(c, h):
        lines = rows_half(h)
        return remote(work.at[2 + mate, lines], cx.at[c, lines], cx_send.at[c, h], cx_recv.at[c, h], mate_at)

    def chunk_of(t):
        return ORDER[t] if isinstance(t, int) else 2 - t + 3 * (t // 2)

    def sum_send(t, h):
        d = chunk_of(t)
        lines = rows_half(h)
        return remote(
            work.at[4 + t % 2, lines], rs.at[d - 1, lines],
            rs_send.at[d - 1, h], rs_recv.at[d - 1, h], place(chip_at(d), core),
        )

    def direct_load(t):
        c = chunk_of(t)
        own = isinstance(t, int) and c == 0
        at = [UPWARD.index((c, b)) if isinstance(t, int) else 1 + 2 * t + b for b in (0, 1)]

        @pl.when(active)
        def _():
            q = chip_at(c)

            @pl.when(jnp.logical_and(r == last, is_down))
            def _():
                for b in (0, 1):
                    block_wait(at[b])

            def load(src, b):
                return pltpu.make_async_copy(src, work.at[0, pl.ds(b * span, span)], local.at[b])

            @pl.when(is_down)
            def _():
                for b in (0, 1):
                    load(pg.at[at[b]], b).start()

            @pl.when(is_home)
            def _():
                for b in (0, 1):
                    if not own:
                        load(ag.at[q, b, pl.ds(part, span)], b).start()
                    else:
                        @pl.when(core == b)
                        def _(b=b):
                            load(panel.at[pl.ds(part, span)], b).start()

                        @pl.when(core != b)
                        def _(b=b):
                            load(ag.at[q, b, pl.ds(part, span)], b).start()

            for b in (0, 1):
                load(pg.at[0], b).wait()

            @pl.loop(0, span // TILE)
            def _(i):
                lines = pl.ds(pl.multiple_of(i * TILE, TILE), TILE)
                for b in (0, 1):
                    big, small = split(work[0, pl.ds(pl.multiple_of(b * span + i * TILE, TILE), TILE)])
                    pgb[lines, b * LANES:(b + 1) * LANES] = big
                    pgb[lines, (2 + b) * LANES:(3 + b) * LANES] = small

    def direct(c, h, begin=0, end=2):
        @pl.when(active)
        def _():
            steps = full // TILE // 4

            @pl.loop((2 * h + begin) * steps, (2 * h + end) * steps)
            def _(i):
                lines = pl.ds(pl.multiple_of(i * TILE, TILE), TILE)
                both = dot(high[lines], pgb[...])
                rest = dot(low[lines], pgb[:, :2 * LANES])
                value = both[:, :2 * LANES] + both[:, 2 * LANES:] + rest
                work[2, lines] = value[:, :LANES]
                work[3, lines] = value[:, LANES:]

        if end == 2:
            trade(c, h).start()

    def direct_sum(t, h):
        c = chunk_of(t)
        own = isinstance(t, int) and c == 0
        slot = 2 + core if own else 4 + t % 2
        if not own:
            @pl.when(t == 2)
            def _():
                sum_send(0, h).wait_send()

        trade(c, h).wait_recv()
        load = pltpu.make_async_copy(cx.at[c, rows_half(h)], work.at[1, rows_half(h)], local.at[2])
        load.start()
        load.wait()
        steps = full // TILE // 2

        @pl.loop(h * steps, (h + 1) * steps)
        def _(i):
            lines = pl.ds(pl.multiple_of(i * TILE, TILE), TILE)
            work[slot, lines] = work[2 + core, lines] + work[1, lines]

        if not own:
            sum_send(t, h).start()
        trade(c, h).wait_send()

    def direct_rest(t):
        direct(chunk_of(t), 1, 0, 1)
        direct_sum(t, 0)
        direct(chunk_of(t), 1, 1, 2)
        direct_sum(t, 1)

    def mirror_task(n, during, after):
        mirror_load(n)
        mirror(n, 0)
        during()
        mirror(n, 1)
        after()

    def direct_task(n, during, after):
        direct_load(n)
        direct(chunk_of(n), 0)
        during()
        direct_rest(n)
        after()

    def at_slot(slot):
        return functools.partial(service, slot)

    service(0)
    mirror_task(0, at_slot(1), at_slot(2))
    service(3)
    mirror_task(1, at_slot(4), at_slot(5))

    lower = r < last - 1

    @pl.loop(2, 7)
    def _(i):
        def within(first):
            def run():
                for n in range(2, 7):
                    @pl.when(i == n)
                    def _(n=n):
                        service(2 * n + first)
            return run

        turn = jnp.where(lower, i >= 5, jnp.logical_and(i % 2 == 0, i < 5))
        n = jnp.where(lower, i - 3, 1 + i // 2)

        @pl.when(turn)
        def _():
            mirror_load(n)
            mirror(n, 0)

        t = jnp.where(lower, i - 2, (i - 2) // 2)

        @pl.when(jnp.logical_not(turn))
        def _():
            direct_load(t)
            direct(chunk_of(t), 0)

        within(2)()

        @pl.when(turn)
        def _():
            mirror(n, 1)

        @pl.when(jnp.logical_not(turn))
        def _():
            direct_rest(t)

        within(3)()

    direct_task(3, at_slot(16), at_slot(17))
    for slot in range(4 * CHIPS + 2, 4 * CHIPS + 2 + rows):
        service(slot)

    def add_up(sources):
        loads = [pltpu.make_async_copy(src, work.at[n], local.at[n]) for n, src in enumerate(sources)]
        for load in loads:
            load.start()
        for load in loads:
            load.wait()

        @pl.loop(0, full // TILE)
        def _(i):
            lines = pl.ds(pl.multiple_of(i * TILE, TILE), TILE)
            total = work[2 + core, lines]
            for n in range(len(sources)):
                total = total + work[n, lines]
            work[2 + core, lines] = total

    def sum_wait(d):
        for h in (0, 1):
            view = rs.at[d - 1, rows_half(h)]
            remote(view, view, rs_send.at[d - 1, h], rs_recv.at[d - 1, h], mate_at).wait_recv()

    sum_wait(1)
    sum_wait(2)
    add_up((rs.at[0], rs.at[1]))
    sum_wait(3)
    add_up((rs.at[2],))
    for a in range(ratio):
        for h in (0, 1):
            view = uf.at[pl.ds(a * span + h * (span // 2), span // 2)]
            remote(view, view, home_sem.at[0, 0], uf_recv.at[a, h], mate_at).wait_recv()
    add_up((uf,))
    store = pltpu.make_async_copy(work.at[2 + core], out, local.at[5])
    store.start()

    for d, h in own_order:
        own_send(d, h).wait_send()
    for d in (1, 2, 3):
        for h in (0, 1):
            pass_on(d, h).wait_send()
    for h in (0, 1):
        sum_send(1, h).wait_send()
        sum_send(2, h).wait_send()

    @pl.when(jnp.logical_or(is_source, is_relay))
    def _():
        for k in range(2 * CHIPS):
            block_send(pg.at[k], k).wait_send()

    for k in range(2 * CHIPS):
        @pl.when(is_down)
        def _(k=k):
            for b in (0, 1):
                down_send(k, b).wait_send()

        for b in (0, 1):
            sent_home = is_home if k // 2 else jnp.logical_and(is_home, core != b)

            @pl.when(sent_home)
            def _(k=k, b=b):
                home_send(k, b).wait_send()

    store.wait()


def fused(rows, upstream, input_panel):
    full, span = upstream.shape
    width = input_panel.shape[1]
    ratio = full // span
    pieces = 2 * CHIPS
    f32 = jnp.float32
    shapes = [
        (full, width),
        (CHIPS, 2, full, width),
        (pieces, span, width),
        (pieces, 2, span // 2, width),
        (CHIPS - 1, full, width),
        (full, width),
        (CHIPS, full, width),
    ]
    anywhere = pl.BlockSpec(memory_space=pl.ANY)
    dma = pltpu.SemaphoreType.DMA
    results = pl.pallas_call(
        functools.partial(kernel, rows),
        out_shape=[jax.ShapeDtypeStruct(shape, f32) for shape in shapes],
        in_specs=[anywhere] * 2,
        out_specs=[anywhere] * len(shapes),
        scratch_shapes=[
            pltpu.VMEM((full, span), jnp.bfloat16),
            pltpu.VMEM((full, span), jnp.bfloat16),
            pltpu.VMEM((6, full, width), f32),
            pltpu.VMEM((4 * width, full), jnp.bfloat16),
            pltpu.VMEM((span, 4 * width), jnp.bfloat16),
            pltpu.VMEM((pieces, 2, span // 2, width), f32),
            dma((7, 2)),
            dma((CHIPS, 2, 2)),
            dma((pieces,)),
            dma((pieces,)),
            dma((pieces, 2)),
            dma((pieces, 2)),
            dma((pieces, 2)),
            dma((ratio, 2)),
            dma((CHIPS, 2)),
            dma((CHIPS, 2)),
            dma((CHIPS - 1, 2)),
            dma((CHIPS - 1, 2)),
            dma((6,)),
        ],
        compiler_params=pltpu.CompilerParams(
            collective_id=0, has_side_effects=True, vmem_limit_bytes=67043328
        ),
    )(upstream, input_panel)
    return results[0]


def solution(mesh):
    rows = mesh.shape["row"]
    cols, reps = mesh.shape["col"], mesh.shape["rep"]
    placed = P("row", GROUP)

    def body(upstream, input_panel):
        full, span = upstream.shape
        whole_tiles = input_panel.shape[1] == LANES and full % TILE == 0 and span % (2 * TILE) == 0
        if cols == 4 and reps == 2 and full == 2 * span and rows > 1 and whole_tiles:
            return fused(rows, upstream, input_panel)
        return per_device(rows, cols * reps, upstream, input_panel)

    return jax.shard_map(
        body, mesh=mesh, in_specs=(placed, placed), out_specs=placed, check_vma=False
    )
```
